32 devices in a mesh: wide: 8 (over z, y), narrow: 4 (over x, core).
Axes of the slice: x: 2, y: 2, z: 4, core: 2. Of those that a mesh axis runs over, the one named last changes fastest.
Arguments:
- values: float32 [512, 16384], P(('wide', 'narrow')), may hold values from -200 to 200, as said below
- cloud_words: int32 [512, 512], P(('wide', 'narrow')), may hold values from -2147483648 to 2147483647, as said below
- history_len: int32 [1], replicated, may hold values from 96 to 256
- monitor_start: int32 [1], replicated, may hold values from 256 to 384
- boundary_table: int32 [512], replicated, may hold values from 500 to 2000
Outputs:
- ratio: float32 [512, 16384], P(('wide', 'narrow'))
- peak_so_far: float32 [512, 16384], P(('wide', 'narrow'))
The draws below stay inside these ranges and needn't reach their ends.
Inputs may be any that keep to these rules, and one draw needn't show every extreme that they name: `values`: values of an index series, mixed noise and a seasonal cycle of varying scale. `cloud_words`: bit b of word j in the row of date t is 1 when pixel 32 j + b is clear at date t; the first 16 dates are clear for every pixel.
All inputs are finite; a program needn't handle non-finite values.
Results may differ from the reference program's by a relative error of at most 0.0003.
Values sent between devices are 32-bit elements; how exact they have to be, the bound alone decides.
A program may use at most 64 MiB of HBM per device.

```python
import math
import jax
import jax.numpy as jnp
from jax import lax

DATES = 512
PIX_DEV = 512
PERIOD = 46
HARMONICS = 3
COLS = 8
WINDOW = 64
PIXELS = 16384


def draw_values(key, part):
    keys = jax.random.split(key, 4)
    day_float = jnp.arange(DATES, dtype=jnp.int32).astype(jnp.float32)[:, None]
    amplitude = jax.random.uniform(keys[2], (PIXELS,), jnp.float32, 0.0, 2.0)
    offset = jax.random.uniform(keys[3], (PIXELS,), jnp.float32, -math.pi, math.pi)
    seasonal = amplitude[None, :] * jnp.cos(2.0 * math.pi / PERIOD * day_float + offset[None, :])
    noise = jnp.clip(jax.random.normal(keys[0], (DATES, PIXELS), jnp.float32), -6.0, 6.0)
    scales = jnp.exp(jax.random.uniform(keys[1], (PIXELS,), jnp.float32, 0.0, math.log(10.0)))
    return scales[None, :] * (noise + seasonal)


def draw_cloud_words(key, part):
    keys = jax.random.split(jax.random.fold_in(key, 17), 2)
    lowest = jnp.iinfo(jnp.int32).min
    highest = jnp.iinfo(jnp.int32).max
    first = jax.random.randint(keys[0], (DATES, PIXELS // 32), lowest, highest, dtype=jnp.int32)
    second = jax.random.randint(keys[1], (DATES, PIXELS // 32), lowest, highest, dtype=jnp.int32)
    words = jnp.bitwise_or(first, second)
    early = (jnp.arange(DATES, dtype=jnp.int32) < 16)[:, None]
    return jnp.where(early, jnp.int32(-1), words)


def with_ends(array, stream_key, smallest, top_value):
    longest = array.shape.index(max(array.shape))
    spots = []
    for shift in (0, 1):
        where = [jax.random.randint(jax.random.fold_in(stream_key, axis), (), 0, length) for axis, length in enumerate(array.shape)]
        where[longest] = (where[longest] + shift) % array.shape[longest]
        spots.append(tuple(where))
    return array.at[spots[0]].set(smallest).at[spots[1]].set(top_value)


def setup_inputs(seed: int = 0) -> dict:
    seeds = jax.random.split(jax.random.key(seed), 6)
    return {
        "values": draw_values(jax.random.fold_in(seeds[5], 71), 0),
        "cloud_words": draw_cloud_words(jax.random.fold_in(seeds[5], 71), 0),
        "history_len": jax.random.randint(seeds[2], (1,), DATES * 3 // 16, DATES // 2 + 1).astype(jnp.int32),
        "monitor_start": jax.random.randint(seeds[3], (1,), DATES // 2, DATES * 3 // 4 + 1).astype(jnp.int32),
        "boundary_table": with_ends(jax.random.randint(seeds[4], (DATES,), 500, 2001), jax.random.fold_in(seeds[4], 1), 500, 2000).astype(jnp.int32),
    }


HIGH = lax.Precision.HIGHEST

def unpack_clear(words):
    shifts = jnp.arange(32, dtype=jnp.int32)
    flags = jnp.bitwise_and(jnp.right_shift(words[:, :, None], shifts[None, None, :]), jnp.int32(1))
    return flags.reshape(words.shape[0], words.shape[1] * 32).astype(jnp.float32)

def harmonic_design(dates):
    day_float = jnp.arange(dates, dtype=jnp.int32).astype(jnp.float32)
    columns = [jnp.ones((dates,), jnp.float32), day_float / dates]
    for harmonic in range(1, HARMONICS + 1):
        phases = 2.0 * math.pi * harmonic / PERIOD * day_float
        columns.append(jnp.cos(phases))
        columns.append(jnp.sin(phases))
    return jnp.stack(columns, axis=1)

def solve_batched(normal_mat, target):
    size_cols = normal_mat.shape[0]
    factor = [[None] * size_cols for row_idx in range(size_cols)]
    for row_idx in range(size_cols):
        for col_idx in range(row_idx + 1):
            summed = normal_mat[row_idx, col_idx]
            for mid_idx in range(col_idx):
                summed = summed - factor[row_idx][mid_idx] * factor[col_idx][mid_idx]
            if row_idx == col_idx:
                factor[row_idx][col_idx] = jnp.sqrt(summed)
            else:
                factor[row_idx][col_idx] = summed / factor[col_idx][col_idx]
    forward = []
    for row_idx in range(size_cols):
        summed = target[row_idx]
        for mid_idx in range(row_idx):
            summed = summed - factor[row_idx][mid_idx] * forward[mid_idx]
        forward.append(summed / factor[row_idx][row_idx])
    solution = [None] * size_cols
    for row_idx in reversed(range(size_cols)):
        summed = forward[row_idx]
        for mid_idx in range(row_idx + 1, size_cols):
            summed = summed - factor[mid_idx][row_idx] * solution[mid_idx]
        solution[row_idx] = summed / factor[row_idx][row_idx]
    return jnp.stack(solution, axis=0)

def fit_statistic(values, clear, history_len, monitor_start, boundary_table):
    dates = values.shape[0]
    day = jnp.arange(dates, dtype=jnp.int32)
    design = harmonic_design(dates)
    in_history = (day < history_len[0]).astype(jnp.float32)[:, None]
    weight = clear * in_history
    outer = (design[:, :, None] * design[:, None, :]).reshape(dates, COLS * COLS)
    normal_mat = jnp.dot(outer.T, weight, precision=HIGH, preferred_element_type=jnp.float32).reshape(COLS, COLS, -1)
    target = jnp.dot(design.T, weight * values, precision=HIGH, preferred_element_type=jnp.float32)
    coeffs = solve_batched(normal_mat, target)
    fitted = jnp.dot(design, coeffs, precision=HIGH, preferred_element_type=jnp.float32)
    resid = clear * (values - fitted)
    count = lax.optimization_barrier(jnp.sum(weight, axis=0))
    squares = lax.optimization_barrier(jnp.sum(weight * resid * resid, axis=0))
    sigma = jnp.sqrt(squares / (count - COLS) + 1e-06)
    lagged = day[:, None] - day[None, :]
    banded = ((lagged >= 0) & (lagged < WINDOW)).astype(jnp.float32)
    moving = jnp.dot(banded, resid, precision=HIGH, preferred_element_type=jnp.float32)
    scaled = moving / (sigma * jnp.sqrt(count))[None, :]
    bounds = boundary_table.astype(jnp.float32) * 0.001
    watching = (day >= monitor_start[0])[:, None]
    return jnp.where(watching, scaled / bounds[:, None], jnp.float32(0.0))

def reassemble(blocked):
    return blocked.transpose(1, 0, 2).reshape(DATES, -1)

def reference(values, cloud_words, history_len, monitor_start, boundary_table):
    block_count = values.shape[1] // PIX_DEV
    value_blocks = values.reshape(DATES, block_count, PIX_DEV).transpose(1, 0, 2)
    word_blocks = cloud_words.reshape(DATES, block_count, PIX_DEV // 32).transpose(1, 0, 2)

    def one_block(block_pair):
        ratio = fit_statistic(block_pair[0], unpack_clear(block_pair[1]), history_len, monitor_start, boundary_table)
        return (ratio, lax.cummax(jnp.abs(ratio), axis=0))
    ratios, peaks = lax.map(one_block, (value_blocks, word_blocks))
    return (reassemble(ratios), reassemble(peaks))
```

```python
import math

import jax
import jax.numpy as jnp
from jax import lax
from jax.sharding import PartitionSpec as P

PERIOD = 46
HARMONICS = 3
COLS = 8
WINDOW = 64


HIGH = lax.Precision.HIGHEST


def unpack_clear(words):
    shifts = jnp.arange(32, dtype=jnp.int32)
    flags = jnp.bitwise_and(jnp.right_shift(words[:, :, None], shifts[None, None, :]), jnp.int32(1))
    return flags.reshape(words.shape[0], words.shape[1] * 32).astype(jnp.float32)


def harmonic_design(dates):
    day_float = jnp.arange(dates, dtype=jnp.int32).astype(jnp.float32)
    columns = [jnp.ones((dates,), jnp.float32), day_float / dates]
    for harmonic in range(1, HARMONICS + 1):
        phases = 2.0 * math.pi * harmonic / PERIOD * day_float
        columns.append(jnp.cos(phases))
        columns.append(jnp.sin(phases))
    return jnp.stack(columns, axis=1)


def solve_batched(normal_mat, target):
    size_cols = normal_mat.shape[0]
    factor = [[None] * size_cols for row_idx in range(size_cols)]
    for row_idx in range(size_cols):
        for col_idx in range(row_idx + 1):
            summed = normal_mat[row_idx, col_idx]
            for mid_idx in range(col_idx):
                summed = summed - factor[row_idx][mid_idx] * factor[col_idx][mid_idx]
            if row_idx == col_idx:
                factor[row_idx][col_idx] = jnp.sqrt(summed)
            else:
                factor[row_idx][col_idx] = summed / factor[col_idx][col_idx]
    forward = []
    for row_idx in range(size_cols):
        summed = target[row_idx]
        for mid_idx in range(row_idx):
            summed = summed - factor[row_idx][mid_idx] * forward[mid_idx]
        forward.append(summed / factor[row_idx][row_idx])
    solution = [None] * size_cols
    for row_idx in reversed(range(size_cols)):
        summed = forward[row_idx]
        for mid_idx in range(row_idx + 1, size_cols):
            summed = summed - factor[mid_idx][row_idx] * solution[mid_idx]
        solution[row_idx] = summed / factor[row_idx][row_idx]
    return jnp.stack(solution, axis=0)


def fit_statistic(values, clear, history_len, monitor_start, boundary_table):
    dates = values.shape[0]
    day = jnp.arange(dates, dtype=jnp.int32)
    design = harmonic_design(dates)
    in_history = (day < history_len[0]).astype(jnp.float32)[:, None]
    weight = clear * in_history
    outer = (design[:, :, None] * design[:, None, :]).reshape(dates, COLS * COLS)
    normal_mat = jnp.dot(
        outer.T, weight, precision=HIGH, preferred_element_type=jnp.float32
    ).reshape(COLS, COLS, -1)
    target = jnp.dot(design.T, weight * values, precision=HIGH, preferred_element_type=jnp.float32)
    coeffs = solve_batched(normal_mat, target)
    fitted = jnp.dot(design, coeffs, precision=HIGH, preferred_element_type=jnp.float32)
    resid = clear * (values - fitted)
    count = jnp.sum(weight, axis=0)
    squares = jnp.sum(weight * resid * resid, axis=0)
    sigma = jnp.sqrt(squares / (count - COLS) + 1e-06)
    lagged = day[:, None] - day[None, :]
    banded = ((lagged >= 0) & (lagged < WINDOW)).astype(jnp.float32)
    moving = jnp.dot(banded, resid, precision=HIGH, preferred_element_type=jnp.float32)
    scaled = moving / (sigma * jnp.sqrt(count))[None, :]
    bounds = boundary_table.astype(jnp.float32) * 0.001
    watching = (day >= monitor_start[0])[:, None]
    return jnp.where(watching, scaled / bounds[:, None], jnp.float32(0.0))


def per_device(values, cloud_words, history_len, monitor_start, boundary_table):
    arrived = lax.all_to_all(values, ("wide", "narrow"), split_axis=1, concat_axis=0, tiled=True)
    words = lax.all_to_all(cloud_words, ("wide", "narrow"), split_axis=1, concat_axis=0, tiled=True)
    ratio = fit_statistic(arrived, unpack_clear(words), history_len, monitor_start, boundary_table)
    rows = values.shape[0]
    blocks = ratio.reshape(ratio.shape[0] // rows, rows, ratio.shape[1])
    block_peak = lax.cummax(jnp.max(jnp.abs(blocks), axis=1), axis=0)
    earlier = jnp.concatenate([jnp.zeros_like(block_peak[:1]), block_peak[:-1]], axis=0)
    date_ratio = lax.all_to_all(ratio, ("wide", "narrow"), split_axis=0, concat_axis=1, tiled=True)
    before = lax.all_to_all(earlier, ("wide", "narrow"), split_axis=0, concat_axis=1, tiled=True)
    peak = jnp.maximum(lax.cummax(jnp.abs(date_ratio), axis=0), before)
    return (date_ratio, peak)


def solution(mesh):
    placed = (P(("wide", "narrow"), None), P(("wide", "narrow"), None), P(), P(), P())
    return jax.shard_map(
        per_device,
        mesh=mesh,
        in_specs=placed,
        out_specs=(P(("wide", "narrow"), None), P(("wide", "narrow"), None)),
        check_vma=False,
    )
```

```python
import functools
import math

import jax
import jax.numpy as jnp
from jax import lax
from jax.experimental import pallas as pl
from jax.experimental.pallas import tpu as pltpu
import numpy as np
from jax.sharding import PartitionSpec as P

PERIOD = 46
HARMONICS = 3
COLS = 8
WINDOW = 64


HIGH = lax.Precision.HIGHEST


def unpack_clear(words):
    shifts = jnp.arange(32, dtype=jnp.int32)
    flags = jnp.bitwise_and(jnp.right_shift(words[:, :, None], shifts[None, None, :]), jnp.int32(1))
    return flags.reshape(words.shape[0], words.shape[1] * 32).astype(jnp.float32)


def harmonic_design(dates):
    day_float = jnp.arange(dates, dtype=jnp.int32).astype(jnp.float32)
    columns = [jnp.ones((dates,), jnp.float32), day_float / dates]
    for harmonic in range(1, HARMONICS + 1):
        phases = 2.0 * math.pi * harmonic / PERIOD * day_float
        columns.append(jnp.cos(phases))
        columns.append(jnp.sin(phases))
    return jnp.stack(columns, axis=1)


def solve_batched(normal_mat, target):
    size_cols = normal_mat.shape[0]
    factor = [[None] * size_cols for row_idx in range(size_cols)]
    for row_idx in range(size_cols):
        for col_idx in range(row_idx + 1):
            summed = normal_mat[row_idx, col_idx]
            for mid_idx in range(col_idx):
                summed = summed - factor[row_idx][mid_idx] * factor[col_idx][mid_idx]
            if row_idx == col_idx:
                factor[row_idx][col_idx] = jnp.sqrt(summed)
            else:
                factor[row_idx][col_idx] = summed / factor[col_idx][col_idx]
    forward = []
    for row_idx in range(size_cols):
        summed = target[row_idx]
        for mid_idx in range(row_idx):
            summed = summed - factor[row_idx][mid_idx] * forward[mid_idx]
        forward.append(summed / factor[row_idx][row_idx])
    solution = [None] * size_cols
    for row_idx in reversed(range(size_cols)):
        summed = forward[row_idx]
        for mid_idx in range(row_idx + 1, size_cols):
            summed = summed - factor[mid_idx][row_idx] * solution[mid_idx]
        solution[row_idx] = summed / factor[row_idx][row_idx]
    return jnp.stack(solution, axis=0)


def fit_statistic(values, clear, history_len, monitor_start, boundary_table):
    dates = values.shape[0]
    day = jnp.arange(dates, dtype=jnp.int32)
    design = harmonic_design(dates)
    in_history = (day < history_len[0]).astype(jnp.float32)[:, None]
    weight = clear * in_history
    outer = (design[:, :, None] * design[:, None, :]).reshape(dates, COLS * COLS)
    normal_mat = jnp.dot(
        outer.T, weight, precision=HIGH, preferred_element_type=jnp.float32
    ).reshape(COLS, COLS, -1)
    target = jnp.dot(design.T, weight * values, precision=HIGH, preferred_element_type=jnp.float32)
    coeffs = solve_batched(normal_mat, target)
    fitted = jnp.dot(design, coeffs, precision=HIGH, preferred_element_type=jnp.float32)
    resid = clear * (values - fitted)
    count = jnp.sum(weight, axis=0)
    squares = jnp.sum(weight * resid * resid, axis=0)
    sigma = jnp.sqrt(squares / (count - COLS) + 1e-06)
    lagged = day[:, None] - day[None, :]
    banded = ((lagged >= 0) & (lagged < WINDOW)).astype(jnp.float32)
    moving = jnp.dot(banded, resid, precision=HIGH, preferred_element_type=jnp.float32)
    scaled = moving / (sigma * jnp.sqrt(count))[None, :]
    bounds = boundary_table.astype(jnp.float32) * 0.001
    watching = (day >= monitor_start[0])[:, None]
    return jnp.where(watching, scaled / bounds[:, None], jnp.float32(0.0))


def per_device(values, cloud_words, history_len, monitor_start, boundary_table):
    arrived = lax.all_to_all(values, ("wide", "narrow"), split_axis=1, concat_axis=0, tiled=True)
    words = lax.all_to_all(cloud_words, ("wide", "narrow"), split_axis=1, concat_axis=0, tiled=True)
    ratio = fit_statistic(arrived, unpack_clear(words), history_len, monitor_start, boundary_table)
    rows = values.shape[0]
    blocks = ratio.reshape(ratio.shape[0] // rows, rows, ratio.shape[1])
    block_peak = lax.cummax(jnp.max(jnp.abs(blocks), axis=1), axis=0)
    earlier = jnp.concatenate([jnp.zeros_like(block_peak[:1]), block_peak[:-1]], axis=0)
    date_ratio = lax.all_to_all(ratio, ("wide", "narrow"), split_axis=0, concat_axis=1, tiled=True)
    before = lax.all_to_all(earlier, ("wide", "narrow"), split_axis=0, concat_axis=1, tiled=True)
    peak = jnp.maximum(lax.cummax(jnp.abs(date_ratio), axis=0), before)
    return (date_ratio, peak)


HISTORY_MOST = 256
MESH = pl.DeviceIdType.MESH


def host_design(dates):
    day = np.arange(dates, dtype=np.float32)
    columns = [np.ones((dates,), np.float32), (day / np.float32(dates)).astype(np.float32)]
    for harmonic in range(1, HARMONICS + 1):
        phases = (np.float32(2.0 * math.pi * harmonic / PERIOD) * day).astype(np.float64)
        columns.append(np.cos(phases).astype(np.float32))
        columns.append(np.sin(phases).astype(np.float32))
    return np.stack(columns, axis=1)


def dot_high(left, right):
    return jnp.dot(left, right, precision=HIGH, preferred_element_type=jnp.float32)


def clear_bits(words, offset, pixels):
    rows, lanes = words.shape
    parts = [((words >> (8 * k)) & 255).astype(jnp.float32).astype(jnp.bfloat16) for k in range(4)]
    stacked = jnp.concatenate(parts, axis=0)
    word_of = lax.broadcasted_iota(jnp.int32, (lanes, pixels), 1) >> 5
    spread = (lax.broadcasted_iota(jnp.int32, (lanes, pixels), 0) - offset == word_of)
    spread = spread.astype(jnp.float32).astype(jnp.bfloat16)
    wide = jnp.dot(stacked, spread, preferred_element_type=jnp.float32)
    lane = lax.broadcasted_iota(jnp.int32, (rows, pixels), 1)
    which = (lane >> 3) & 3
    byte = wide[:rows]
    for k in range(1, 4):
        byte = jnp.where(which == k, wide[k * rows : (k + 1) * rows], byte)
    return ((byte.astype(jnp.int32) >> (lane & 7)) & 1).astype(jnp.float32)


def scan_rows(array, combine, neutral):
    rows = array.shape[0]
    row = lax.broadcasted_iota(jnp.int32, array.shape, 0)
    step = 1
    while step < rows:
        shifted = jnp.where(row >= step, pltpu.roll(array, step, 0), neutral)
        array = combine(array, shifted)
        step *= 2
    return array


def solve_rows(entry, target):
    factor = [[None] * COLS for _ in range(COLS)]
    inverse = [None] * COLS
    for i in range(COLS):
        for j in range(i + 1):
            summed = entry(i, j)
            for m in range(j):
                summed = summed - factor[i][m] * factor[j][m]
            if i == j:
                inverse[i] = 1.0 / jnp.sqrt(summed)
            else:
                factor[i][j] = summed * inverse[j]
    forward = []
    for i in range(COLS):
        summed = target(i)
        for m in range(i):
            summed = summed - factor[i][m] * forward[m]
        forward.append(summed * inverse[i])
    answer = [None] * COLS
    for i in reversed(range(COLS)):
        summed = forward[i]
        for m in range(i + 1, COLS):
            summed = summed - factor[m][i] * answer[m]
        answer[i] = summed * inverse[i]
    return answer


def fused_kernel(
    narrow, chips, hist, back,
    hl_ref, ms_ref, v_ref, w_ref, d_ref, dt_ref, ot_ref, b_ref, ratio_ref, peak_ref,
    cv, cw, ccl, hv, hw, ow, tp, tb, nm, cb, cnt, sq, sb, tot, tt, sc, scb, rt, mrow, mb,
    ax_s, ax_r, ha_s, ha_r, hw_s, hw_r, ow_s, ow_r, tp_s, tp_r, cb_s, cb_r, ct_s, ct_r,
    sq_s, sq_r, tt_s, tt_r, sc_s, sc_r, mx_s, mx_r, or_s, or_r, op_s, op_r, lc,
):
    me = lax.axis_index("wide") * narrow + lax.axis_index("narrow")
    q, c = lax.div(me, 2), lax.rem(me, 2)
    rows, pixels = v_ref.shape
    half = pixels // 2
    own = half // hist
    slots = hist
    chip_rows = 2 * rows
    late = chips - hist
    is_hist = q < hist
    is_late = q >= hist

    def dev(q2, c2):
        d = 2 * q2 + c2
        return (lax.div(d, narrow), lax.rem(d, narrow))

    def remote(src, dst, ssem, rsem, q2, c2):
        return pltpu.make_async_remote_copy(
            src_ref=src, dst_ref=dst, send_sem=ssem, recv_sem=rsem,
            device_id=dev(q2, c2), device_id_type=MESH)

    def cols(s):
        return pl.ds(pl.multiple_of(s * own, own), own)

    mine = pl.ds(pl.multiple_of(c * rows, rows), rows)
    theirs = pl.ds(pl.multiple_of((1 - c) * rows, rows), rows)
    my_half = pl.ds(pl.multiple_of(c * half, half), half)
    other_half = pl.ds(pl.multiple_of((1 - c) * half, half), half)

    def half_col(h, s):
        return pl.ds(pl.multiple_of(h * half + s * own, own), own)

    swap_v = remote(v_ref.at[:, other_half], cv.at[mine, :], ax_s.at[0], ax_r.at[0], q, 1 - c)
    swap_w = remote(w_ref, cw.at[mine, :], ax_s.at[1], ax_r.at[1], q, 1 - c)
    swap_w.start()
    swap_v.start()
    keep_v = pltpu.make_async_copy(v_ref.at[:, my_half], cv.at[mine, :], lc.at[0])
    keep_w = pltpu.make_async_copy(w_ref, cw.at[mine, :], lc.at[1])
    keep_v.start()
    keep_w.start()

    def owner_block(q2, c2):
        return pl.ds(pl.multiple_of(lax.div(c2 * half + q2 * own, 32 * 128) * 128, 128), 128)

    my_dates = pl.ds(pl.multiple_of(me * rows, rows), rows)
    keep_o = pltpu.make_async_copy(w_ref.at[:, owner_block(q, c)], ow.at[my_dates, :], lc.at[2])

    def send_words(k):
        to = lax.rem(me + k, 2 * hist)
        return remote(w_ref.at[:, owner_block(lax.div(to, 2), lax.rem(to, 2))],
                      ow.at[my_dates, :], ow_s.at[k - 1], ow_r.at[k - 1],
                      lax.div(to, 2), lax.rem(to, 2))

    @pl.when(is_hist)
    def _():
        @pl.loop(1, 2 * hist)
        def _(k):
            send_words(k).start()
        keep_o.start()

    sends_early = jnp.logical_and(q + back >= hist, q + back < chips)

    def early_words(h):
        return remote(w_ref, hw.at[mine, :], hw_s.at[h], hw_r.at[c], q + back, h)

    def early(h, s):
        return remote(v_ref.at[:, half_col(h, s)], hv.at[mine, cols(s)],
                      ha_s.at[h * slots + s], ha_r.at[c * slots + s], q + back, h)

    @pl.when(sends_early)
    def _():
        for h in range(2):
            early_words(h).start()

        @pl.loop(0, slots)
        def _(s):
            early(0, s).start()
            early(1, s).start()

    def word_block(s):
        start = c * (half // 32) + s * (own // 32)
        base = lax.div(start, 128) * 128
        return pl.ds(pl.multiple_of(base, 128), 128), start - base

    keep_w.wait()
    swap_w.wait_recv()

    @pl.loop(0, slots)
    def _(s):
        block, offset = word_block(s)
        ccl[:, cols(s)] = clear_bits(cw[:, block], offset, own)

    keep_v.wait()
    swap_v.wait_recv()
    date = q * chip_rows + lax.broadcasted_iota(jnp.int32, (chip_rows, own), 0)

    def send_target(k):
        to = lax.rem(q + k, hist)
        return remote(tp.at[to], tb.at[q], tp_s.at[k - 1], tp_r.at[k - 1], to, c)

    def send_coeffs(k, base):
        return remote(cb.at[q - base], cb.at[q - base], cb_s.at[k - 1], cb_r.at[k - 1],
                      base + lax.rem(q - base + k, hist), c)

    relay = remote(cb.at[q], cb.at[q], cb_s.at[hist - 1], cb_r.at[hist - 1], q + hist, c)
    give_count = remote(cnt, cnt, ct_s.at[0], ct_r.at[0], q + hist, c)

    @pl.when(is_hist)
    def _():
        @pl.loop(0, slots)
        def _(s):
            weighted = jnp.where(date < hl_ref[0], ccl[:, cols(s)] * cv[:, cols(s)], 0.0)
            tp[s] = dot_high(dt_ref[q], weighted)

        @pl.loop(1, hist)
        def _(k):
            send_target(k).start()

        ratio_ref[...] = jnp.zeros_like(ratio_ref)
        peak_ref[...] = jnp.zeros_like(peak_ref)
        keep_o.wait()

        @pl.loop(1, 2 * hist)
        def _(k):
            send_words(k).wait_recv()

        start = c * (half // 32) + q * (own // 32)
        flags = clear_bits(ow[...], lax.rem(start, 128), own)
        day = lax.broadcasted_iota(jnp.int32, flags.shape, 0)
        nm[...] = dot_high(ot_ref[...], jnp.where(day < hl_ref[0], flags, 0.0))
        cnt[...] = nm[0:1, :]
        give_count.start()
        total = tp[q]

        @pl.loop(1, hist)
        def _(k):
            send_target(k).wait_recv()

        tb[q] = total
        total = tb[0]
        for s in range(1, hist):
            total = total + tb[s]
        tb[q] = total

        def entry(i, j):
            at = i * (i + 1) // 2 + j
            return nm[at : at + 1, :]

        answer = solve_rows(entry, lambda i: tb[q, i : i + 1, :])
        for i in range(COLS):
            cb[q, i : i + 1, :] = answer[i]
        relay.start()

        @pl.loop(1, hist)
        def _(k):
            send_coeffs(k, 0).start()

        @pl.loop(1, hist)
        def _(k):
            send_coeffs(k, 0).wait_recv()

    @pl.when(is_late)
    def _():
        for h in range(2):
            remote(w_ref, hw.at[pl.ds(h * rows, rows), :], hw_s.at[h], hw_r.at[h], q, 1 - c).wait_recv()
        remote(cb.at[q - hist], cb.at[q - hist], cb_s.at[hist - 1], cb_r.at[hist - 1], q - hist, c).wait_recv()

        @pl.loop(1, hist)
        def _(k):
            send_coeffs(k, hist).start()

        @pl.loop(1, hist)
        def _(k):
            send_coeffs(k, hist).wait_recv()

    @pl.loop(0, slots)
    def _(s):
        resid = ccl[:, cols(s)] * (cv[:, cols(s)] - dot_high(d_ref[q], cb[s]))
        cv[:, cols(s)] = resid
        tot[0:1, cols(s)] = jnp.sum(resid, axis=0, keepdims=True)
        sq[s] = jnp.sum(jnp.where(date < hl_ref[0], resid * resid, 0.0), axis=0, keepdims=True)

    def send_total(j):
        return remote(tot, tt.at[j - 1], tt_s.at[j - 1], tt_r.at[j - 1], q + j, c)

    for j in range(1, back):
        @pl.when(jnp.logical_and(q + j >= hist, q + j < chips))
        def _():
            send_total(j).start()

    def send_squares(s):
        return remote(sq.at[s], sb.at[q], sq_s.at[s], sq_r.at[q], hist + s, c)

    @pl.when(is_hist)
    def _():
        @pl.loop(0, hist)
        def _(k):
            send_squares(lax.rem(q + k, hist)).start()

    def send_scale(k):
        return remote(sc, scb.at[q - hist], sc_s.at[k - 1], sc_r.at[k - 1],
                      hist + lax.rem(q - hist + k, hist), c)

    def send_max(s, k):
        return remote(mrow.at[s], mb.at[q - hist, s], mx_s.at[s * late + k], mx_r.at[s * late + q - hist], hist + k, c)

    def ratio_out(s):
        return remote(rt.at[theirs, cols(s)], ratio_ref.at[:, half_col(c, s)], or_s.at[s], or_r.at[s], q, 1 - c)

    def peak_out(s):
        return remote(hv.at[theirs, cols(s)], peak_ref.at[:, half_col(c, s)], op_s.at[s], op_r.at[s], q, 1 - c)

    @pl.when(is_late)
    def _():
        @pl.loop(0, hist)
        def _(s):
            remote(sq.at[s], sb.at[s], sq_s.at[s], sq_r.at[s], q - hist, c).wait_recv()
        give_count.wait_recv()
        squares = sb[0]
        for s in range(1, hist):
            squares = squares + sb[s]
        count = cnt[...]
        sigma = jnp.sqrt(squares / (count - COLS) + 1e-06)
        scale = 1.0 / (sigma * jnp.sqrt(count))
        sc[...] = scale
        scb[q - hist] = scale

        @pl.loop(1, hist)
        def _(k):
            send_scale(k).start()

        @pl.loop(1, hist)
        def _(k):
            send_scale(k).wait_recv()

        for j in range(1, back):
            send_total(j).wait_recv()

        row = lax.broadcasted_iota(jnp.int32, (chip_rows, chip_rows), 0)
        col = lax.broadcasted_iota(jnp.int32, (chip_rows, chip_rows), 1)
        upto = (col <= row).astype(jnp.float32)
        after = (col > row).astype(jnp.float32)
        bounds = b_ref[q].astype(jnp.float32) * 0.001

        @pl.loop(0, slots)
        def _(s):
            for h in range(2):
                remote(v_ref.at[:, half_col(h, s)], hv.at[pl.ds(h * rows, rows), cols(s)],
                       ha_s.at[h * slots + s], ha_r.at[h * slots + s], q, 1 - c).wait_recv()
            block, offset = word_block(s)
            flags = clear_bits(hw[:, block], offset, own)
            early_resid = flags * (hv[:, cols(s)] - dot_high(d_ref[q - back], cb[s]))
            moving = dot_high(upto, cv[:, cols(s)]) + dot_high(after, early_resid)
            for j in range(1, back):
                moving = moving + tt[j - 1, 0:1, cols(s)]
            ratio = jnp.where(date >= ms_ref[0], moving * scb[s] / bounds, 0.0)
            rt[:, cols(s)] = ratio
            best = scan_rows(jnp.abs(ratio), jnp.maximum, 0.0)
            ccl[:, cols(s)] = best
            mrow[s] = best[chip_rows - 1 :, :]

            @pl.loop(q - hist + 1, late)
            def _(k):
                send_max(s, k).start()

            ratio_out(s).start()
            ratio_ref[:, half_col(c, s)] = rt[mine, cols(s)]

        @pl.loop(0, slots)
        def _(s):
            def earlier(k, best):
                remote(mrow.at[s], mb.at[k, s], mx_s.at[s * late + k], mx_r.at[s * late + k], q, 1 - c).wait_recv()
                return jnp.maximum(best, mb[k, s])

            before = lax.fori_loop(0, q - hist, earlier, jnp.zeros((1, own), jnp.float32))
            hv[:, cols(s)] = jnp.maximum(ccl[:, cols(s)], before)
            peak_out(s).start()
            peak_ref[:, half_col(c, s)] = hv[mine, cols(s)]

        @pl.loop(0, slots)
        def _(s):
            ratio_out(s).wait()
            peak_out(s).wait()

            @pl.loop(q - hist + 1, late)
            def _(k):
                send_max(s, k).wait_send()

        @pl.loop(1, hist)
        def _(k):
            send_scale(k).wait_send()
            send_coeffs(k, hist).wait_send()

    swap_v.wait_send()
    swap_w.wait_send()

    @pl.when(is_hist)
    def _():
        @pl.loop(1, 2 * hist)
        def _(k):
            send_words(k).wait_send()

        @pl.loop(1, hist)
        def _(k):
            send_target(k).wait_send()
            send_coeffs(k, 0).wait_send()

        relay.wait_send()
        give_count.wait_send()

        @pl.loop(0, hist)
        def _(s):
            send_squares(s).wait_send()

    @pl.when(sends_early)
    def _():
        for h in range(2):
            early_words(h).wait_send()

        @pl.loop(0, slots)
        def _(s):
            early(0, s).wait_send()
            early(1, s).wait_send()

    for j in range(1, back):
        @pl.when(jnp.logical_and(q + j >= hist, q + j < chips))
        def _():
            send_total(j).wait_send()


def fused_device(narrow, devices, values, cloud_words, history_len, monitor_start, boundary_table):
    rows, pixels = values.shape
    chips, chip_rows, half = devices // 2, 2 * rows, pixels // 2
    dates = boundary_table.shape[0]
    hist, back = HISTORY_MOST // chip_rows, WINDOW // chip_rows
    own, late = half // hist, chips - hist
    design = host_design(dates)
    lower = [(i, j) for i in range(COLS) for j in range(i + 1)]
    outer = np.zeros((40, HISTORY_MOST), np.float32)
    for at, (i, j) in enumerate(lower):
        outer[at] = design[:HISTORY_MOST, i] * design[:HISTORY_MOST, j]
    by_chip = design.reshape(chips, chip_rows, COLS)
    vmem = pl.BlockSpec(memory_space=pltpu.VMEM)
    smem = pl.BlockSpec(memory_space=pltpu.SMEM)
    f32, i32, dma = jnp.float32, jnp.int32, pltpu.SemaphoreType.DMA
    scratch = [
        pltpu.VMEM((chip_rows, half), f32),
        pltpu.VMEM((chip_rows, pixels // 32), i32),
        pltpu.VMEM((chip_rows, half), f32),
        pltpu.VMEM((chip_rows, half), f32),
        pltpu.VMEM((chip_rows, pixels // 32), i32),
        pltpu.VMEM((HISTORY_MOST, 128), i32),
        pltpu.VMEM((hist, COLS, own), f32),
        pltpu.VMEM((hist, COLS, own), f32),
        pltpu.VMEM((40, own), f32),
        pltpu.VMEM((hist, COLS, own), f32),
        pltpu.VMEM((1, own), f32),
        pltpu.VMEM((hist, 1, own), f32),
        pltpu.VMEM((hist, 1, own), f32),
        pltpu.VMEM((1, half), f32),
        pltpu.VMEM((max(back - 1, 1), 1, half), f32),
        pltpu.VMEM((1, own), f32),
        pltpu.VMEM((hist, 1, own), f32),
        pltpu.VMEM((chip_rows, half), f32),
        pltpu.VMEM((hist, 1, own), f32),
        pltpu.VMEM((late, hist, 1, own), f32),
    ]
    for number in (2, 2 * hist, 2, 2 * hist, hist, hist, 1, hist, max(back - 1, 1), hist, hist * late, hist, hist):
        scratch += [dma((number,)), dma((number,))]
    scratch.append(dma((3,)))
    return pl.pallas_call(
        functools.partial(fused_kernel, narrow, chips, hist, back),
        out_shape=[jax.ShapeDtypeStruct((rows, pixels), f32)] * 2,
        in_specs=[smem, smem] + [vmem] * 6,
        out_specs=[vmem, vmem],
        scratch_shapes=scratch,
        compiler_params=pltpu.CompilerParams(has_side_effects=True, vmem_limit_bytes=40 * 1024 * 1024),
    )(
        history_len, monitor_start, values, cloud_words, jnp.asarray(by_chip),
        jnp.asarray(by_chip.transpose(0, 2, 1)), jnp.asarray(outer),
        boundary_table.reshape(chips, chip_rows, 1),
    )


def fits(narrow, devices, rows, pixels):
    chip_rows = 2 * rows
    if narrow % 2 or rows % 8 or HISTORY_MOST % chip_rows or WINDOW % chip_rows:
        return False
    hist = HISTORY_MOST // chip_rows
    return devices // 2 == 2 * hist and (pixels // 2) % (hist * 128) == 0 and 128 % (pixels // 64 // hist) == 0


def solution(mesh):
    narrow = mesh.shape["narrow"]
    devices = narrow * mesh.shape["wide"]

    def per_device_any(values, *rest):
        if fits(narrow, devices, *values.shape):
            return fused_device(narrow, devices, values, *rest)
        return per_device(values, *rest)

    placed = (P(("wide", "narrow"), None), P(("wide", "narrow"), None), P(), P(), P())
    return jax.shard_map(
        per_device_any,
        mesh=mesh,
        in_specs=placed,
        out_specs=(P(("wide", "narrow"), None), P(("wide", "narrow"), None)),
        check_vma=False,
    )
```

```python
import functools
import math

import jax
import jax.numpy as jnp
from jax import lax
from jax.experimental import pallas as pl
from jax.experimental.pallas import tpu as pltpu
import numpy as np
from jax.sharding import PartitionSpec as P

PERIOD = 46
HARMONICS = 3
COLS = 8
WINDOW = 64


HIGH = lax.Precision.HIGHEST


def unpack_clear(words):
    shifts = jnp.arange(32, dtype=jnp.int32)
    flags = jnp.bitwise_and(jnp.right_shift(words[:, :, None], shifts[None, None, :]), jnp.int32(1))
    return flags.reshape(words.shape[0], words.shape[1] * 32).astype(jnp.float32)


def harmonic_design(dates):
    day_float = jnp.arange(dates, dtype=jnp.int32).astype(jnp.float32)
    columns = [jnp.ones((dates,), jnp.float32), day_float / dates]
    for harmonic in range(1, HARMONICS + 1):
        phases = 2.0 * math.pi * harmonic / PERIOD * day_float
        columns.append(jnp.cos(phases))
        columns.append(jnp.sin(phases))
    return jnp.stack(columns, axis=1)


def solve_batched(normal_mat, target):
    size_cols = normal_mat.shape[0]
    factor = [[None] * size_cols for row_idx in range(size_cols)]
    for row_idx in range(size_cols):
        for col_idx in range(row_idx + 1):
            summed = normal_mat[row_idx, col_idx]
            for mid_idx in range(col_idx):
                summed = summed - factor[row_idx][mid_idx] * factor[col_idx][mid_idx]
            if row_idx == col_idx:
                factor[row_idx][col_idx] = jnp.sqrt(summed)
            else:
                factor[row_idx][col_idx] = summed / factor[col_idx][col_idx]
    forward = []
    for row_idx in range(size_cols):
        summed = target[row_idx]
        for mid_idx in range(row_idx):
            summed = summed - factor[row_idx][mid_idx] * forward[mid_idx]
        forward.append(summed / factor[row_idx][row_idx])
    solution = [None] * size_cols
    for row_idx in reversed(range(size_cols)):
        summed = forward[row_idx]
        for mid_idx in range(row_idx + 1, size_cols):
            summed = summed - factor[mid_idx][row_idx] * solution[mid_idx]
        solution[row_idx] = summed / factor[row_idx][row_idx]
    return jnp.stack(solution, axis=0)


def fit_statistic(values, clear, history_len, monitor_start, boundary_table):
    dates = values.shape[0]
    day = jnp.arange(dates, dtype=jnp.int32)
    design = harmonic_design(dates)
    in_history = (day < history_len[0]).astype(jnp.float32)[:, None]
    weight = clear * in_history
    outer = (design[:, :, None] * design[:, None, :]).reshape(dates, COLS * COLS)
    normal_mat = jnp.dot(
        outer.T, weight, precision=HIGH, preferred_element_type=jnp.float32
    ).reshape(COLS, COLS, -1)
    target = jnp.dot(design.T, weight * values, precision=HIGH, preferred_element_type=jnp.float32)
    coeffs = solve_batched(normal_mat, target)
    fitted = jnp.dot(design, coeffs, precision=HIGH, preferred_element_type=jnp.float32)
    resid = clear * (values - fitted)
    count = jnp.sum(weight, axis=0)
    squares = jnp.sum(weight * resid * resid, axis=0)
    sigma = jnp.sqrt(squares / (count - COLS) + 1e-06)
    lagged = day[:, None] - day[None, :]
    banded = ((lagged >= 0) & (lagged < WINDOW)).astype(jnp.float32)
    moving = jnp.dot(banded, resid, precision=HIGH, preferred_element_type=jnp.float32)
    scaled = moving / (sigma * jnp.sqrt(count))[None, :]
    bounds = boundary_table.astype(jnp.float32) * 0.001
    watching = (day >= monitor_start[0])[:, None]
    return jnp.where(watching, scaled / bounds[:, None], jnp.float32(0.0))


def per_device(values, cloud_words, history_len, monitor_start, boundary_table):
    arrived = lax.all_to_all(values, ("wide", "narrow"), split_axis=1, concat_axis=0, tiled=True)
    words = lax.all_to_all(cloud_words, ("wide", "narrow"), split_axis=1, concat_axis=0, tiled=True)
    ratio = fit_statistic(arrived, unpack_clear(words), history_len, monitor_start, boundary_table)
    rows = values.shape[0]
    blocks = ratio.reshape(ratio.shape[0] // rows, rows, ratio.shape[1])
    block_peak = lax.cummax(jnp.max(jnp.abs(blocks), axis=1), axis=0)
    earlier = jnp.concatenate([jnp.zeros_like(block_peak[:1]), block_peak[:-1]], axis=0)
    date_ratio = lax.all_to_all(ratio, ("wide", "narrow"), split_axis=0, concat_axis=1, tiled=True)
    before = lax.all_to_all(earlier, ("wide", "narrow"), split_axis=0, concat_axis=1, tiled=True)
    peak = jnp.maximum(lax.cummax(jnp.abs(date_ratio), axis=0), before)
    return (date_ratio, peak)


HISTORY_MOST = 256
MESH = pl.DeviceIdType.MESH


def host_design(dates):
    day = np.arange(dates, dtype=np.float32)
    columns = [np.ones((dates,), np.float32), (day / np.float32(dates)).astype(np.float32)]
    for harmonic in range(1, HARMONICS + 1):
        phases = (np.float32(2.0 * math.pi * harmonic / PERIOD) * day).astype(np.float64)
        columns.append(np.cos(phases).astype(np.float32))
        columns.append(np.sin(phases).astype(np.float32))
    return np.stack(columns, axis=1)


def dot_high(left, right):
    return jnp.dot(left, right, precision=HIGH, preferred_element_type=jnp.float32)


def clear_bits(words, offset, pixels):
    rows, lanes = words.shape
    parts = [((words >> (8 * k)) & 255).astype(jnp.float32).astype(jnp.bfloat16) for k in range(4)]
    stacked = jnp.concatenate(parts, axis=0)
    word_of = lax.broadcasted_iota(jnp.int32, (lanes, pixels), 1) >> 5
    spread = (lax.broadcasted_iota(jnp.int32, (lanes, pixels), 0) - offset == word_of)
    spread = spread.astype(jnp.float32).astype(jnp.bfloat16)
    wide = jnp.dot(stacked, spread, preferred_element_type=jnp.float32)
    lane = lax.broadcasted_iota(jnp.int32, (rows, pixels), 1)
    which = (lane >> 3) & 3
    byte = wide[:rows]
    for k in range(1, 4):
        byte = jnp.where(which == k, wide[k * rows : (k + 1) * rows], byte)
    return ((byte.astype(jnp.int32) >> (lane & 7)) & 1).astype(jnp.float32)


def scan_rows(array, combine, neutral):
    tiles = []
    row = lax.broadcasted_iota(jnp.int32, (8, array.shape[1]), 0)
    for at in range(0, array.shape[0], 8):
        tile = array[at : at + 8]
        for step in (1, 2, 4):
            tile = combine(tile, jnp.where(row >= step, pltpu.roll(tile, step, 0), neutral))
        if tiles:
            tile = combine(tile, tiles[-1][7:8])
        tiles.append(tile)
    return jnp.concatenate(tiles, axis=0)


def fitted(design, coeffs):
    total = design[:, 0:1] * coeffs[0:1]
    for k in range(1, COLS):
        total = total + design[:, k : k + 1] * coeffs[k : k + 1]
    return total


def solve_rows(entry, target):
    factor = [[None] * COLS for _ in range(COLS)]
    inverse = [None] * COLS
    for i in range(COLS):
        for j in range(i + 1):
            summed = entry(i, j)
            for m in range(j):
                summed = summed - factor[i][m] * factor[j][m]
            if i == j:
                inverse[i] = 1.0 / jnp.sqrt(summed)
            else:
                factor[i][j] = summed * inverse[j]
    forward = []
    for i in range(COLS):
        summed = target(i)
        for m in range(i):
            summed = summed - factor[i][m] * forward[m]
        forward.append(summed * inverse[i])
    answer = [None] * COLS
    for i in reversed(range(COLS)):
        summed = forward[i]
        for m in range(i + 1, COLS):
            summed = summed - factor[m][i] * answer[m]
        answer[i] = summed * inverse[i]
    return answer


def fused_kernel(
    narrow, chips, hist, back,
    hl_ref, ms_ref, b_ref, v_ref, w_ref, d_hbm, ot_hbm, ratio_ref, peak_ref,
    cv, cw, ccl, hv, hw, ow, tp, tb, nm, cb, cnt, sq, sb, tot, tt, sc, scb, rt, mrow, mb, rin, pin, dm, de, ot_ref,
    ax_s, ax_r, ha_s, ha_r, hw_s, hw_r, ow_s, ow_r, tp_s, tp_r, cb_s, cb_r, ct_s, ct_r,
    sq_s, sq_r, tt_s, tt_r, sc_s, sc_r, mx_s, mx_r, or_s, or_r, op_s, op_r, lc,
):
    me = lax.axis_index("wide") * narrow + lax.axis_index("narrow")
    q, c = lax.div(me, 2), lax.rem(me, 2)
    rows, pixels = v_ref.shape
    half = pixels // 2
    own = half // hist
    slots = hist
    chip_rows = 2 * rows
    late = chips - hist
    is_hist = q < hist
    is_late = q >= hist

    def dev(q2, c2):
        d = 2 * q2 + c2
        return (lax.div(d, narrow), lax.rem(d, narrow))

    def remote(src, dst, ssem, rsem, q2, c2):
        return pltpu.make_async_remote_copy(
            src_ref=src, dst_ref=dst, send_sem=ssem, recv_sem=rsem,
            device_id=dev(q2, c2), device_id_type=MESH)

    def cols(s):
        return pl.ds(pl.multiple_of(s * own, own), own)

    mine = pl.ds(pl.multiple_of(c * rows, rows), rows)
    theirs = pl.ds(pl.multiple_of((1 - c) * rows, rows), rows)
    my_half = pl.ds(pl.multiple_of(c * half, half), half)
    other_half = pl.ds(pl.multiple_of((1 - c) * half, half), half)

    def half_col(h, s):
        return pl.ds(pl.multiple_of(h * half + s * own, own), own)

    swap_v = remote(v_ref.at[:, other_half], cv.at[mine, :], ax_s.at[0], ax_r.at[0], q, 1 - c)
    swap_w = remote(w_ref, cw.at[mine, :], ax_s.at[1], ax_r.at[1], q, 1 - c)
    swap_w.start()
    swap_v.start()
    get_d = pltpu.make_async_copy(d_hbm.at[q], dm, lc.at[3])
    get_e = pltpu.make_async_copy(d_hbm.at[lax.max(q - back, 0)], de, lc.at[4])
    get_o = pltpu.make_async_copy(ot_hbm, ot_ref, lc.at[5])
    get_d.start()
    get_e.start()
    get_o.start()
    keep_v = pltpu.make_async_copy(v_ref.at[:, my_half], cv.at[mine, :], lc.at[0])
    keep_w = pltpu.make_async_copy(w_ref, cw.at[mine, :], lc.at[1])
    keep_v.start()
    keep_w.start()

    def owner_block(q2, c2):
        return pl.ds(pl.multiple_of(lax.div(c2 * half + q2 * own, 32 * 128) * 128, 128), 128)

    my_dates = pl.ds(pl.multiple_of(me * rows, rows), rows)
    keep_o = pltpu.make_async_copy(w_ref.at[:, owner_block(q, c)], ow.at[my_dates, :], lc.at[2])

    def send_words(k):
        to = lax.rem(me + k, 2 * hist)
        return remote(w_ref.at[:, owner_block(lax.div(to, 2), lax.rem(to, 2))],
                      ow.at[my_dates, :], ow_s.at[k - 1], ow_r.at[k - 1],
                      lax.div(to, 2), lax.rem(to, 2))

    @pl.when(is_hist)
    def _():
        @pl.loop(1, 2 * hist)
        def _(k):
            send_words(k).start()
        keep_o.start()

    sends_early = jnp.logical_and(q + back >= hist, q + back < chips)

    def early_words(h):
        return remote(w_ref, hw.at[mine, :], hw_s.at[h], hw_r.at[c], q + back, h)

    def early(h, s):
        return remote(v_ref.at[:, half_col(h, s)], hv.at[mine, cols(s)],
                      ha_s.at[h * slots + s], ha_r.at[c * slots + s], q + back, h)

    third, most = slots // 4, slots * 5 // 8

    def start_early(low, high):
        @pl.when(sends_early)
        def _():
            @pl.loop(low, high)
            def _(s):
                early(0, s).start()
                early(1, s).start()

    @pl.when(sends_early)
    def _():
        for h in range(2):
            early_words(h).start()

    start_early(0, third)

    @pl.when(is_late)
    def _():
        start_early(third, most)

    def word_block(s):
        start = c * (half // 32) + s * (own // 32)
        base = lax.div(start, 128) * 128
        return pl.ds(pl.multiple_of(base, 128), 128), start - base

    keep_w.wait()
    swap_w.wait_recv()

    @pl.loop(0, slots)
    def _(s):
        block, offset = word_block(s)
        ccl[:, cols(s)] = clear_bits(cw[:, block], offset, own)

    keep_v.wait()
    swap_v.wait_recv()
    get_d.wait()
    get_e.wait()
    get_o.wait()
    date = q * chip_rows + lax.broadcasted_iota(jnp.int32, (chip_rows, own), 0)

    def send_target(k):
        to = lax.rem(q + k, hist)
        return remote(tp.at[to], tb.at[q], tp_s.at[k - 1], tp_r.at[k - 1], to, c)

    def send_coeffs(k, base):
        return remote(cb.at[q - base], cb.at[q - base], cb_s.at[k - 1], cb_r.at[k - 1],
                      base + lax.rem(q - base + k, hist), c)

    relay = remote(cb.at[q], cb.at[q], cb_s.at[hist - 1], cb_r.at[hist - 1], q + hist, c)
    give_count = remote(cnt, cnt, ct_s.at[0], ct_r.at[0], q + hist, c)

    @pl.when(is_hist)
    def _():
        @pl.loop(0, slots)
        def _(s):
            weighted = jnp.where(date < hl_ref[0], ccl[:, cols(s)] * cv[:, cols(s)], 0.0)
            for k in range(COLS):
                tp[s, k : k + 1, :] = jnp.sum(weighted * dm[:, k : k + 1], axis=0, keepdims=True)

        @pl.loop(1, hist)
        def _(k):
            send_target(k).start()

        start_early(third, most)
        ratio_ref[...] = jnp.zeros_like(ratio_ref)
        peak_ref[...] = jnp.zeros_like(peak_ref)
        keep_o.wait()

        @pl.loop(1, 2 * hist)
        def _(k):
            send_words(k).wait_recv()

        start = c * (half // 32) + q * (own // 32)
        flags = clear_bits(ow[...], lax.rem(start, 128), own)
        day = lax.broadcasted_iota(jnp.int32, flags.shape, 0)
        nm[...] = dot_high(ot_ref[...], jnp.where(day < hl_ref[0], flags, 0.0))
        cnt[...] = nm[0:1, :]
        give_count.start()
        total = tp[q]

        @pl.loop(1, hist)
        def _(k):
            send_target(k).wait_recv()

        tb[q] = total
        total = tb[0]
        for s in range(1, hist):
            total = total + tb[s]
        tb[q] = total

        def entry(i, j):
            at = i * (i + 1) // 2 + j
            return nm[at : at + 1, :]

        answer = solve_rows(entry, lambda i: tb[q, i : i + 1, :])
        for i in range(COLS):
            cb[q, i : i + 1, :] = answer[i]
        relay.start()

        @pl.loop(1, hist)
        def _(k):
            send_coeffs(k, 0).start()

        start_early(most, slots)

        @pl.loop(1, hist)
        def _(k):
            send_coeffs(k, 0).wait_recv()

    @pl.when(is_late)
    def _():
        for h in range(2):
            remote(w_ref, hw.at[pl.ds(h * rows, rows), :], hw_s.at[h], hw_r.at[h], q, 1 - c).wait_recv()

        @pl.loop(0, slots)
        def _(s):
            block, offset = word_block(s)
            rt[:, cols(s)] = clear_bits(hw[:, block], offset, own)

        remote(cb.at[q - hist], cb.at[q - hist], cb_s.at[hist - 1], cb_r.at[hist - 1], q - hist, c).wait_recv()

        @pl.loop(1, hist)
        def _(k):
            send_coeffs(k, hist).start()

        start_early(most, slots)

        @pl.loop(1, hist)
        def _(k):
            send_coeffs(k, hist).wait_recv()

    @pl.loop(0, slots)
    def _(s):
        resid = ccl[:, cols(s)] * (cv[:, cols(s)] - fitted(dm[...], cb[s]))
        cv[:, cols(s)] = resid
        tot[0:1, cols(s)] = jnp.sum(resid, axis=0, keepdims=True)
        sq[s] = jnp.sum(jnp.where(date < hl_ref[0], resid * resid, 0.0), axis=0, keepdims=True)

    def send_total(j):
        return remote(tot, tt.at[j - 1], tt_s.at[j - 1], tt_r.at[j - 1], q + j, c)

    for j in range(1, back):
        @pl.when(jnp.logical_and(q + j >= hist, q + j < chips))
        def _():
            send_total(j).start()

    def send_squares(s):
        return remote(sq.at[s], sb.at[q], sq_s.at[s], sq_r.at[q], hist + s, c)

    @pl.when(is_hist)
    def _():
        @pl.loop(0, hist)
        def _(k):
            send_squares(lax.rem(q + k, hist)).start()

    def send_scale(k):
        to = lax.rem(me - 2 * hist + k, 2 * late)
        return remote(sc, scb.at[c, q - hist], sc_s.at[k - 1], sc_r.at[k - 1],
                      hist + lax.div(to, 2), lax.rem(to, 2))

    def send_max(s, k):
        return remote(mrow.at[s], mb.at[q - hist, s], mx_s.at[s * late + k], mx_r.at[s * late + q - hist], hist + k, c)

    def ratio_out(s):
        return remote(rt.at[theirs, cols(s)], rin.at[:, cols(s)], or_s.at[s], or_r.at[s], q, 1 - c)

    def peak_out(s):
        return remote(hv.at[theirs, cols(s)], pin.at[:, cols(s)], op_s.at[s], op_r.at[s], q, 1 - c)

    @pl.when(is_late)
    def _():
        row = lax.broadcasted_iota(jnp.int32, (chip_rows, 128), 0)
        bounds = jnp.zeros((chip_rows, 128), jnp.int32)
        for i in range(chip_rows):
            bounds = jnp.where(row == i, b_ref[q * chip_rows + i], bounds)
        over = 1.0 / (bounds[:, 0:1].astype(jnp.float32) * 0.001)

        @pl.loop(0, slots)
        def _(s):
            for h in range(2):
                remote(v_ref.at[:, half_col(h, s)], hv.at[pl.ds(h * rows, rows), cols(s)],
                       ha_s.at[h * slots + s], ha_r.at[h * slots + s], q, 1 - c).wait_recv()
            early_resid = rt[:, cols(s)] * (hv[:, cols(s)] - fitted(de[...], cb[s]))
            change = cv[:, cols(s)] - early_resid
            rt[:, cols(s)] = scan_rows(change, jnp.add, 0.0) + jnp.sum(early_resid, axis=0, keepdims=True)

        for j in range(1, back):
            send_total(j).wait_recv()

        @pl.loop(0, slots)
        def _(s):
            moving = rt[:, cols(s)]
            for j in range(1, back):
                moving = moving + tt[j - 1, 0:1, cols(s)]
            ratio = jnp.where(date >= ms_ref[0], moving * over, 0.0)
            rt[:, cols(s)] = ratio
            best = scan_rows(jnp.abs(ratio), jnp.maximum, 0.0)
            ccl[:, cols(s)] = best
            mrow[s] = best[chip_rows - 1 :, :]

            @pl.loop(q - hist + 1, late)
            def _(k):
                send_max(s, k).start()

            ratio_out(s).start()

        @pl.loop(0, hist)
        def _(s):
            remote(sq.at[s], sb.at[s], sq_s.at[s], sq_r.at[s], q - hist, c).wait_recv()
        give_count.wait_recv()
        squares = sb[0]
        for s in range(1, hist):
            squares = squares + sb[s]
        count = cnt[...]
        sigma = jnp.sqrt(squares / (count - COLS) + 1e-06)
        scale = 1.0 / (sigma * jnp.sqrt(count))
        sc[...] = scale
        scb[c, q - hist] = scale

        @pl.loop(1, 2 * late)
        def _(k):
            send_scale(k).start()

        @pl.loop(0, slots)
        def _(s):
            def earlier(k, best):
                remote(mrow.at[s], mb.at[k, s], mx_s.at[s * late + k], mx_r.at[s * late + k], q, 1 - c).wait_recv()
                return jnp.maximum(best, mb[k, s])

            before = lax.fori_loop(0, q - hist, earlier, jnp.zeros((1, own), jnp.float32))
            hv[:, cols(s)] = jnp.maximum(ccl[:, cols(s)], before)
            peak_out(s).start()

        @pl.loop(1, 2 * late)
        def _(k):
            send_scale(k).wait_recv()

        @pl.loop(0, slots)
        def _(s):
            scale = scb[c, s]
            ratio_ref[:, half_col(c, s)] = rt[mine, cols(s)] * scale
            peak_ref[:, half_col(c, s)] = hv[mine, cols(s)] * scale

        @pl.loop(0, slots)
        def _(s):
            ratio_out(s).wait_recv()
            peak_out(s).wait_recv()
            scale = scb[1 - c, s]
            ratio_ref[:, half_col(1 - c, s)] = rin[:, cols(s)] * scale
            peak_ref[:, half_col(1 - c, s)] = pin[:, cols(s)] * scale

        @pl.loop(0, slots)
        def _(s):
            ratio_out(s).wait_send()
            peak_out(s).wait_send()

            @pl.loop(q - hist + 1, late)
            def _(k):
                send_max(s, k).wait_send()

        @pl.loop(1, 2 * late)
        def _(k):
            send_scale(k).wait_send()

        @pl.loop(1, hist)
        def _(k):
            send_coeffs(k, hist).wait_send()

    swap_v.wait_send()
    swap_w.wait_send()

    @pl.when(is_hist)
    def _():
        @pl.loop(1, 2 * hist)
        def _(k):
            send_words(k).wait_send()

        @pl.loop(1, hist)
        def _(k):
            send_target(k).wait_send()
            send_coeffs(k, 0).wait_send()

        relay.wait_send()
        give_count.wait_send()

        @pl.loop(0, hist)
        def _(s):
            send_squares(s).wait_send()

    @pl.when(sends_early)
    def _():
        for h in range(2):
            early_words(h).wait_send()

        @pl.loop(0, slots)
        def _(s):
            early(0, s).wait_send()
            early(1, s).wait_send()

    for j in range(1, back):
        @pl.when(jnp.logical_and(q + j >= hist, q + j < chips))
        def _():
            send_total(j).wait_send()


def fused_device(narrow, devices, values, cloud_words, history_len, monitor_start, boundary_table):
    rows, pixels = values.shape
    chips, chip_rows, half = devices // 2, 2 * rows, pixels // 2
    dates = boundary_table.shape[0]
    hist, back = HISTORY_MOST // chip_rows, WINDOW // chip_rows
    own, late = half // hist, chips - hist
    design = host_design(dates)
    lower = [(i, j) for i in range(COLS) for j in range(i + 1)]
    outer = np.zeros((40, HISTORY_MOST), np.float32)
    for at, (i, j) in enumerate(lower):
        outer[at] = design[:HISTORY_MOST, i] * design[:HISTORY_MOST, j]
    by_chip = design.reshape(chips, chip_rows, COLS)
    vmem = pl.BlockSpec(memory_space=pltpu.VMEM)
    hbm = pl.BlockSpec(memory_space=pl.ANY)
    smem = pl.BlockSpec(memory_space=pltpu.SMEM)
    f32, i32, dma = jnp.float32, jnp.int32, pltpu.SemaphoreType.DMA
    scratch = [
        pltpu.VMEM((chip_rows, half), f32),
        pltpu.VMEM((chip_rows, pixels // 32), i32),
        pltpu.VMEM((chip_rows, half), f32),
        pltpu.VMEM((chip_rows, half), f32),
        pltpu.VMEM((chip_rows, pixels // 32), i32),
        pltpu.VMEM((HISTORY_MOST, 128), i32),
        pltpu.VMEM((hist, COLS, own), f32),
        pltpu.VMEM((hist, COLS, own), f32),
        pltpu.VMEM((40, own), f32),
        pltpu.VMEM((hist, COLS, own), f32),
        pltpu.VMEM((1, own), f32),
        pltpu.VMEM((hist, 1, own), f32),
        pltpu.VMEM((hist, 1, own), f32),
        pltpu.VMEM((1, half), f32),
        pltpu.VMEM((max(back - 1, 1), 1, half), f32),
        pltpu.VMEM((1, own), f32),
        pltpu.VMEM((2, late, 1, own), f32),
        pltpu.VMEM((chip_rows, half), f32),
        pltpu.VMEM((hist, 1, own), f32),
        pltpu.VMEM((late, hist, 1, own), f32),
        pltpu.VMEM((rows, half), f32),
        pltpu.VMEM((rows, half), f32),
        pltpu.VMEM((chip_rows, COLS), f32),
        pltpu.VMEM((chip_rows, COLS), f32),
        pltpu.VMEM((40, HISTORY_MOST), f32),
    ]
    for number in (2, 2 * hist, 2, 2 * hist, hist, hist, 1, hist, max(back - 1, 1), 2 * late, hist * late, hist, hist):
        scratch += [dma((number,)), dma((number,))]
    scratch.append(dma((6,)))
    return pl.pallas_call(
        functools.partial(fused_kernel, narrow, chips, hist, back),
        out_shape=[jax.ShapeDtypeStruct((rows, pixels), f32)] * 2,
        in_specs=[smem, smem, smem, vmem, vmem, hbm, hbm],
        out_specs=[vmem, vmem],
        scratch_shapes=scratch,
        compiler_params=pltpu.CompilerParams(has_side_effects=True, vmem_limit_bytes=40 * 1024 * 1024),
    )(
        history_len, monitor_start, boundary_table, values, cloud_words,
        jnp.asarray(by_chip), jnp.asarray(outer),
    )


def fits(narrow, devices, rows, pixels):
    chip_rows = 2 * rows
    if narrow % 2 or rows % 8 or HISTORY_MOST % chip_rows or WINDOW % chip_rows:
        return False
    hist = HISTORY_MOST // chip_rows
    return devices // 2 == 2 * hist and (pixels // 2) % (hist * 128) == 0 and 128 % (pixels // 64 // hist) == 0


def solution(mesh):
    narrow = mesh.shape["narrow"]
    devices = narrow * mesh.shape["wide"]

    def per_device_any(values, *rest):
        if fits(narrow, devices, *values.shape):
            return fused_device(narrow, devices, values, *rest)
        return per_device(values, *rest)

    placed = (P(("wide", "narrow"), None), P(("wide", "narrow"), None), P(), P(), P())
    return jax.shard_map(
        per_device_any,
        mesh=mesh,
        in_specs=placed,
        out_specs=(P(("wide", "narrow"), None), P(("wide", "narrow"), None)),
        check_vma=False,
    )
```

```python
import functools
import math

import jax
import jax.numpy as jnp
from jax import lax
from jax.experimental import pallas as pl
from jax.experimental.pallas import tpu as pltpu
import numpy as np
from jax.sharding import PartitionSpec as P

PERIOD = 46
HARMONICS = 3
COLS = 8
WINDOW = 64


HIGH = lax.Precision.HIGHEST


def unpack_clear(words):
    shifts = jnp.arange(32, dtype=jnp.int32)
    flags = jnp.bitwise_and(jnp.right_shift(words[:, :, None], shifts[None, None, :]), jnp.int32(1))
    return flags.reshape(words.shape[0], words.shape[1] * 32).astype(jnp.float32)


def harmonic_design(dates):
    day_float = jnp.arange(dates, dtype=jnp.int32).astype(jnp.float32)
    columns = [jnp.ones((dates,), jnp.float32), day_float / dates]
    for harmonic in range(1, HARMONICS + 1):
        phases = 2.0 * math.pi * harmonic / PERIOD * day_float
        columns.append(jnp.cos(phases))
        columns.append(jnp.sin(phases))
    return jnp.stack(columns, axis=1)


def solve_batched(normal_mat, target):
    size_cols = normal_mat.shape[0]
    factor = [[None] * size_cols for row_idx in range(size_cols)]
    for row_idx in range(size_cols):
        for col_idx in range(row_idx + 1):
            summed = normal_mat[row_idx, col_idx]
            for mid_idx in range(col_idx):
                summed = summed - factor[row_idx][mid_idx] * factor[col_idx][mid_idx]
            if row_idx == col_idx:
                factor[row_idx][col_idx] = jnp.sqrt(summed)
            else:
                factor[row_idx][col_idx] = summed / factor[col_idx][col_idx]
    forward = []
    for row_idx in range(size_cols):
        summed = target[row_idx]
        for mid_idx in range(row_idx):
            summed = summed - factor[row_idx][mid_idx] * forward[mid_idx]
        forward.append(summed / factor[row_idx][row_idx])
    solution = [None] * size_cols
    for row_idx in reversed(range(size_cols)):
        summed = forward[row_idx]
        for mid_idx in range(row_idx + 1, size_cols):
            summed = summed - factor[mid_idx][row_idx] * solution[mid_idx]
        solution[row_idx] = summed / factor[row_idx][row_idx]
    return jnp.stack(solution, axis=0)


def fit_statistic(values, clear, history_len, monitor_start, boundary_table):
    dates = values.shape[0]
    day = jnp.arange(dates, dtype=jnp.int32)
    design = harmonic_design(dates)
    in_history = (day < history_len[0]).astype(jnp.float32)[:, None]
    weight = clear * in_history
    outer = (design[:, :, None] * design[:, None, :]).reshape(dates, COLS * COLS)
    normal_mat = jnp.dot(
        outer.T, weight, precision=HIGH, preferred_element_type=jnp.float32
    ).reshape(COLS, COLS, -1)
    target = jnp.dot(design.T, weight * values, precision=HIGH, preferred_element_type=jnp.float32)
    coeffs = solve_batched(normal_mat, target)
    fitted = jnp.dot(design, coeffs, precision=HIGH, preferred_element_type=jnp.float32)
    resid = clear * (values - fitted)
    count = jnp.sum(weight, axis=0)
    squares = jnp.sum(weight * resid * resid, axis=0)
    sigma = jnp.sqrt(squares / (count - COLS) + 1e-06)
    lagged = day[:, None] - day[None, :]
    banded = ((lagged >= 0) & (lagged < WINDOW)).astype(jnp.float32)
    moving = jnp.dot(banded, resid, precision=HIGH, preferred_element_type=jnp.float32)
    scaled = moving / (sigma * jnp.sqrt(count))[None, :]
    bounds = boundary_table.astype(jnp.float32) * 0.001
    watching = (day >= monitor_start[0])[:, None]
    return jnp.where(watching, scaled / bounds[:, None], jnp.float32(0.0))


def per_device(values, cloud_words, history_len, monitor_start, boundary_table):
    arrived = lax.all_to_all(values, ("wide", "narrow"), split_axis=1, concat_axis=0, tiled=True)
    words = lax.all_to_all(cloud_words, ("wide", "narrow"), split_axis=1, concat_axis=0, tiled=True)
    ratio = fit_statistic(arrived, unpack_clear(words), history_len, monitor_start, boundary_table)
    rows = values.shape[0]
    blocks = ratio.reshape(ratio.shape[0] // rows, rows, ratio.shape[1])
    block_peak = lax.cummax(jnp.max(jnp.abs(blocks), axis=1), axis=0)
    earlier = jnp.concatenate([jnp.zeros_like(block_peak[:1]), block_peak[:-1]], axis=0)
    date_ratio = lax.all_to_all(ratio, ("wide", "narrow"), split_axis=0, concat_axis=1, tiled=True)
    before = lax.all_to_all(earlier, ("wide", "narrow"), split_axis=0, concat_axis=1, tiled=True)
    peak = jnp.maximum(lax.cummax(jnp.abs(date_ratio), axis=0), before)
    return (date_ratio, peak)


HISTORY_MOST = 256
MESH = pl.DeviceIdType.MESH


def host_design(dates):
    day = np.arange(dates, dtype=np.float32)
    columns = [np.ones((dates,), np.float32), (day / np.float32(dates)).astype(np.float32)]
    for harmonic in range(1, HARMONICS + 1):
        phases = (np.float32(2.0 * math.pi * harmonic / PERIOD) * day).astype(np.float64)
        columns.append(np.cos(phases).astype(np.float32))
        columns.append(np.sin(phases).astype(np.float32))
    return np.stack(columns, axis=1)


def dot_high(left, right):
    return jnp.dot(left, right, precision=HIGH, preferred_element_type=jnp.float32)


def clear_bits(words, offset, pixels):
    rows, lanes = words.shape
    parts = [((words >> (8 * k)) & 255).astype(jnp.float32).astype(jnp.bfloat16) for k in range(4)]
    stacked = jnp.concatenate(parts, axis=0)
    word_of = lax.broadcasted_iota(jnp.int32, (lanes, pixels), 1) >> 5
    spread = (lax.broadcasted_iota(jnp.int32, (lanes, pixels), 0) - offset == word_of)
    spread = spread.astype(jnp.float32).astype(jnp.bfloat16)
    wide = jnp.dot(stacked, spread, preferred_element_type=jnp.float32)
    lane = lax.broadcasted_iota(jnp.int32, (rows, pixels), 1)
    which = (lane >> 3) & 3
    byte = wide[:rows]
    for k in range(1, 4):
        byte = jnp.where(which == k, wide[k * rows : (k + 1) * rows], byte)
    return ((byte.astype(jnp.int32) >> (lane & 7)) & 1).astype(jnp.float32)


def scan_rows(array, combine, neutral):
    tiles = []
    row = lax.broadcasted_iota(jnp.int32, (8, array.shape[1]), 0)
    for at in range(0, array.shape[0], 8):
        tile = array[at : at + 8]
        for step in (1, 2, 4):
            tile = combine(tile, jnp.where(row >= step, pltpu.roll(tile, step, 0), neutral))
        if tiles:
            tile = combine(tile, tiles[-1][7:8])
        tiles.append(tile)
    return jnp.concatenate(tiles, axis=0)


def fitted(design, coeffs):
    total = design[:, 0:1] * coeffs[0:1]
    for k in range(1, COLS):
        total = total + design[:, k : k + 1] * coeffs[k : k + 1]
    return total


def solve_rows(entry, target):
    factor = [[None] * COLS for _ in range(COLS)]
    inverse = [None] * COLS
    for i in range(COLS):
        for j in range(i + 1):
            summed = entry(i, j)
            for m in range(j):
                summed = summed - factor[i][m] * factor[j][m]
            if i == j:
                inverse[i] = 1.0 / jnp.sqrt(summed)
            else:
                factor[i][j] = summed * inverse[j]
    forward = []
    for i in range(COLS):
        summed = target(i)
        for m in range(i):
            summed = summed - factor[i][m] * forward[m]
        forward.append(summed * inverse[i])
    answer = [None] * COLS
    for i in reversed(range(COLS)):
        summed = forward[i]
        for m in range(i + 1, COLS):
            summed = summed - factor[m][i] * answer[m]
        answer[i] = summed * inverse[i]
    return answer


def fused_kernel(
    narrow, chips, hist, back,
    hl_ref, ms_ref, b_ref, v_ref, w_ref, d_hbm, ot_hbm, ratio_ref, peak_ref,
    cv, cw, ccl, hv, hw, ow, tp, tb, nm, cb, cnt, sq, sb, tot, tt, sc, scb, rt, mrow, mb, rin, pin, dm, de, ot_ref,
    ax_s, ax_r, ha_s, ha_r, hw_s, hw_r, ow_s, ow_r, tp_s, tp_r, cb_s, cb_r, ct_s, ct_r,
    sq_s, sq_r, tt_s, tt_r, sc_s, sc_r, mx_s, mx_r, or_s, or_r, op_s, op_r, lc,
):
    me = lax.axis_index("wide") * narrow + lax.axis_index("narrow")
    q, c = lax.div(me, 2), lax.rem(me, 2)
    rows, pixels = v_ref.shape
    half = pixels // 2
    own = half // hist
    slots = hist
    chip_rows = 2 * rows
    late = chips - hist
    is_hist = q < hist
    is_late = q >= hist

    def dev(q2, c2):
        d = 2 * q2 + c2
        return (lax.div(d, narrow), lax.rem(d, narrow))

    def remote(src, dst, ssem, rsem, q2, c2):
        return pltpu.make_async_remote_copy(
            src_ref=src, dst_ref=dst, send_sem=ssem, recv_sem=rsem,
            device_id=dev(q2, c2), device_id_type=MESH)

    def cols(s):
        return pl.ds(pl.multiple_of(s * own, own), own)

    mine = pl.ds(pl.multiple_of(c * rows, rows), rows)
    theirs = pl.ds(pl.multiple_of((1 - c) * rows, rows), rows)
    my_half = pl.ds(pl.multiple_of(c * half, half), half)
    other_half = pl.ds(pl.multiple_of((1 - c) * half, half), half)

    def half_col(h, s):
        return pl.ds(pl.multiple_of(h * half + s * own, own), own)

    swap_v = remote(v_ref.at[:, other_half], cv.at[mine, :], ax_s.at[0], ax_r.at[0], q, 1 - c)
    swap_w = remote(w_ref, cw.at[mine, :], ax_s.at[1], ax_r.at[1], q, 1 - c)
    swap_w.start()
    swap_v.start()
    get_d = pltpu.make_async_copy(d_hbm.at[q], dm, lc.at[3])
    get_e = pltpu.make_async_copy(d_hbm.at[lax.max(q - back, 0)], de, lc.at[4])
    get_o = pltpu.make_async_copy(ot_hbm, ot_ref, lc.at[5])
    get_d.start()
    get_e.start()
    get_o.start()
    keep_v = pltpu.make_async_copy(v_ref.at[:, my_half], cv.at[mine, :], lc.at[0])
    keep_w = pltpu.make_async_copy(w_ref, cw.at[mine, :], lc.at[1])
    keep_v.start()
    keep_w.start()

    def owner_block(q2, c2):
        return pl.ds(pl.multiple_of(lax.div(c2 * half + q2 * own, 32 * 128) * 128, 128), 128)

    my_dates = pl.ds(pl.multiple_of(me * rows, rows), rows)
    keep_o = pltpu.make_async_copy(w_ref.at[:, owner_block(q, c)], ow.at[my_dates, :], lc.at[2])

    def send_words(k):
        to = lax.rem(me + k, 2 * hist)
        return remote(w_ref.at[:, owner_block(lax.div(to, 2), lax.rem(to, 2))],
                      ow.at[my_dates, :], ow_s.at[k - 1], ow_r.at[k - 1],
                      lax.div(to, 2), lax.rem(to, 2))

    @pl.when(is_hist)
    def _():
        @pl.loop(1, 2 * hist)
        def _(k):
            send_words(k).start()
        keep_o.start()

    sends_early = jnp.logical_and(q + back >= hist, q + back < chips)

    def early_words(h):
        return remote(w_ref, hw.at[mine, :], hw_s.at[h], hw_r.at[c], q + back, h)

    def early(h, s):
        return remote(v_ref.at[:, half_col(h, s)], hv.at[mine, cols(s)],
                      ha_s.at[h * slots + s], ha_r.at[c * slots + s], q + back, h)

    third, most = slots // 4, slots * 5 // 8

    def start_early(low, high):
        @pl.when(sends_early)
        def _():
            @pl.loop(low, high)
            def _(s):
                early(0, s).start()
                early(1, s).start()

    @pl.when(sends_early)
    def _():
        for h in range(2):
            early_words(h).start()

    start_early(0, third)

    @pl.when(is_late)
    def _():
        start_early(third, most)

    def word_block(s):
        start = c * (half // 32) + s * (own // 32)
        base = lax.div(start, 128) * 128
        return pl.ds(pl.multiple_of(base, 128), 128), start - base

    keep_w.wait()
    swap_w.wait_recv()

    @pl.loop(0, slots)
    def _(s):
        block, offset = word_block(s)
        ccl[:, cols(s)] = clear_bits(cw[:, block], offset, own)

    keep_v.wait()
    swap_v.wait_recv()
    get_d.wait()
    get_e.wait()
    get_o.wait()
    date = q * chip_rows + lax.broadcasted_iota(jnp.int32, (chip_rows, own), 0)

    def send_target(k):
        to = lax.rem(q + k, hist)
        return remote(tp.at[to], tb.at[q], tp_s.at[k - 1], tp_r.at[k - 1], to, c)

    def send_coeffs(k, base):
        return remote(cb.at[q - base], cb.at[q - base], cb_s.at[k - 1], cb_r.at[k - 1],
                      base + lax.rem(q - base + k, hist), c)

    relay = remote(cb.at[q], cb.at[q], cb_s.at[hist - 1], cb_r.at[hist - 1], q + hist, c)
    give_count = remote(cnt, cnt, ct_s.at[0], ct_r.at[0], q + hist, c)

    @pl.when(is_hist)
    def _():
        @pl.loop(0, slots)
        def _(s):
            weighted = jnp.where(date < hl_ref[0], ccl[:, cols(s)] * cv[:, cols(s)], 0.0)
            for k in range(COLS):
                tp[s, k : k + 1, :] = jnp.sum(weighted * dm[:, k : k + 1], axis=0, keepdims=True)

        @pl.loop(1, hist)
        def _(k):
            send_target(k).start()

        start_early(third, most)
        ratio_ref[...] = jnp.zeros_like(ratio_ref)
        peak_ref[...] = jnp.zeros_like(peak_ref)
        keep_o.wait()

        @pl.loop(1, 2 * hist)
        def _(k):
            send_words(k).wait_recv()

        start = c * (half // 32) + q * (own // 32)
        flags = clear_bits(ow[...], lax.rem(start, 128), own)
        day = lax.broadcasted_iota(jnp.int32, flags.shape, 0)
        nm[...] = dot_high(ot_ref[...], jnp.where(day < hl_ref[0], flags, 0.0))
        cnt[...] = nm[0:1, :]
        give_count.start()
        total = tp[q]

        @pl.loop(1, hist)
        def _(k):
            send_target(k).wait_recv()

        tb[q] = total
        total = tb[0]
        for s in range(1, hist):
            total = total + tb[s]
        tb[q] = total

        def entry(i, j):
            at = i * (i + 1) // 2 + j
            return nm[at : at + 1, :]

        answer = solve_rows(entry, lambda i: tb[q, i : i + 1, :])
        for i in range(COLS):
            cb[q, i : i + 1, :] = answer[i]
        relay.start()

        @pl.loop(1, hist)
        def _(k):
            send_coeffs(k, 0).start()

        start_early(most, slots)

        @pl.loop(1, hist)
        def _(k):
            send_coeffs(k, 0).wait_recv()

    @pl.when(is_late)
    def _():
        for h in range(2):
            remote(w_ref, hw.at[pl.ds(h * rows, rows), :], hw_s.at[h], hw_r.at[h], q, 1 - c).wait_recv()

        @pl.loop(0, slots)
        def _(s):
            block, offset = word_block(s)
            rt[:, cols(s)] = clear_bits(hw[:, block], offset, own)

        remote(cb.at[q - hist], cb.at[q - hist], cb_s.at[hist - 1], cb_r.at[hist - 1], q - hist, c).wait_recv()

        @pl.loop(1, hist)
        def _(k):
            send_coeffs(k, hist).start()

        start_early(most, slots)

        @pl.loop(1, hist)
        def _(k):
            send_coeffs(k, hist).wait_recv()

    @pl.loop(0, slots)
    def _(s):
        resid = ccl[:, cols(s)] * (cv[:, cols(s)] - fitted(dm[...], cb[s]))
        cv[:, cols(s)] = resid
        tot[0:1, cols(s)] = jnp.sum(resid, axis=0, keepdims=True)
        sq[s] = jnp.sum(jnp.where(date < hl_ref[0], resid * resid, 0.0), axis=0, keepdims=True)

    def send_total(j):
        return remote(tot, tt.at[j - 1], tt_s.at[j - 1], tt_r.at[j - 1], q + j, c)

    for j in range(1, back):
        @pl.when(jnp.logical_and(q + j >= hist, q + j < chips))
        def _():
            send_total(j).start()

    def send_squares(s):
        return remote(sq.at[s], sb.at[q], sq_s.at[s], sq_r.at[q], hist + s, c)

    @pl.when(is_hist)
    def _():
        @pl.loop(0, hist)
        def _(k):
            send_squares(lax.rem(q + k, hist)).start()

    def send_scale(k):
        to = lax.rem(me - 2 * hist + k, 2 * late)
        return remote(sc, scb.at[c, q - hist], sc_s.at[k - 1], sc_r.at[k - 1],
                      hist + lax.div(to, 2), lax.rem(to, 2))

    def send_max(s, k):
        return remote(mrow.at[s], mb.at[q - hist, s], mx_s.at[s * late + k], mx_r.at[s * late + q - hist], hist + k, c)

    def ratio_out(s):
        return remote(rt.at[theirs, cols(s)], rin.at[:, cols(s)], or_s.at[s], or_r.at[s], q, 1 - c)

    def peak_out(s):
        return remote(hv.at[theirs, cols(s)], pin.at[:, cols(s)], op_s.at[s], op_r.at[s], q, 1 - c)

    @pl.when(is_late)
    def _():
        row = lax.broadcasted_iota(jnp.int32, (chip_rows, 128), 0)
        bounds = jnp.zeros((chip_rows, 128), jnp.int32)
        for i in range(chip_rows):
            bounds = jnp.where(row == i, b_ref[q * chip_rows + i], bounds)
        over = 1.0 / (bounds[:, 0:1].astype(jnp.float32) * 0.001)

        @pl.loop(0, slots)
        def _(s):
            for h in range(2):
                remote(v_ref.at[:, half_col(h, s)], hv.at[pl.ds(h * rows, rows), cols(s)],
                       ha_s.at[h * slots + s], ha_r.at[h * slots + s], q, 1 - c).wait_recv()
            early_resid = rt[:, cols(s)] * (hv[:, cols(s)] - fitted(de[...], cb[s]))
            change = cv[:, cols(s)] - early_resid
            rt[:, cols(s)] = scan_rows(change, jnp.add, 0.0) + jnp.sum(early_resid, axis=0, keepdims=True)

        for j in range(1, back):
            send_total(j).wait_recv()

        @pl.loop(0, slots)
        def _(s):
            moving = rt[:, cols(s)]
            for j in range(1, back):
                moving = moving + tt[j - 1, 0:1, cols(s)]
            ratio = jnp.where(date >= ms_ref[0], moving * over, 0.0)
            rt[:, cols(s)] = ratio
            best = scan_rows(jnp.abs(ratio), jnp.maximum, 0.0)
            ccl[:, cols(s)] = best
            mrow[s] = best[chip_rows - 1 :, :]

            @pl.loop(q - hist + 1, late)
            def _(k):
                send_max(s, k).start()

            ratio_out(s).start()

        @pl.loop(0, hist)
        def _(s):
            remote(sq.at[s], sb.at[s], sq_s.at[s], sq_r.at[s], q - hist, c).wait_recv()
        give_count.wait_recv()
        squares = sb[0]
        for s in range(1, hist):
            squares = squares + sb[s]
        count = cnt[...]
        sigma = jnp.sqrt(squares / (count - COLS) + 1e-06)
        scale = 1.0 / (sigma * jnp.sqrt(count))
        sc[...] = scale
        scb[c, q - hist] = scale

        @pl.loop(1, 2 * late)
        def _(k):
            send_scale(k).start()

        @pl.loop(0, slots)
        def _(s):
            def earlier(k, best):
                remote(mrow.at[s], mb.at[k, s], mx_s.at[s * late + k], mx_r.at[s * late + k], q, 1 - c).wait_recv()
                return jnp.maximum(best, mb[k, s])

            before = lax.fori_loop(0, q - hist, earlier, jnp.zeros((1, own), jnp.float32))
            hv[:, cols(s)] = jnp.maximum(ccl[:, cols(s)], before)
            peak_out(s).start()

        @pl.loop(1, 2 * late)
        def _(k):
            send_scale(k).wait_recv()

        @pl.loop(0, slots)
        def _(s):
            scale = scb[c, s]
            ratio_ref[:, half_col(c, s)] = rt[mine, cols(s)] * scale
            peak_ref[:, half_col(c, s)] = hv[mine, cols(s)] * scale

        @pl.loop(0, slots)
        def _(s):
            ratio_out(s).wait_recv()
            peak_out(s).wait_recv()
            scale = scb[1 - c, s]
            ratio_ref[:, half_col(1 - c, s)] = rin[:, cols(s)] * scale
            peak_ref[:, half_col(1 - c, s)] = pin[:, cols(s)] * scale

        @pl.loop(0, slots)
        def _(s):
            ratio_out(s).wait_send()
            peak_out(s).wait_send()

            @pl.loop(q - hist + 1, late)
            def _(k):
                send_max(s, k).wait_send()

        @pl.loop(1, 2 * late)
        def _(k):
            send_scale(k).wait_send()

        @pl.loop(1, hist)
        def _(k):
            send_coeffs(k, hist).wait_send()

    swap_v.wait_send()
    swap_w.wait_send()

    @pl.when(is_hist)
    def _():
        @pl.loop(1, 2 * hist)
        def _(k):
            send_words(k).wait_send()

        @pl.loop(1, hist)
        def _(k):
            send_target(k).wait_send()
            send_coeffs(k, 0).wait_send()

        relay.wait_send()
        give_count.wait_send()

        @pl.loop(0, hist)
        def _(s):
            send_squares(s).wait_send()

    @pl.when(sends_early)
    def _():
        for h in range(2):
            early_words(h).wait_send()

        @pl.loop(0, slots)
        def _(s):
            early(0, s).wait_send()
            early(1, s).wait_send()

    for j in range(1, back):
        @pl.when(jnp.logical_and(q + j >= hist, q + j < chips))
        def _():
            send_total(j).wait_send()


def fused_device(narrow, devices, values, cloud_words, history_len, monitor_start, boundary_table):
    rows, pixels = values.shape
    chips, chip_rows, half = devices // 2, 2 * rows, pixels // 2
    dates = boundary_table.shape[0]
    hist, back = HISTORY_MOST // chip_rows, WINDOW // chip_rows
    own, late = half // hist, chips - hist
    design = host_design(dates)
    lower = [(i, j) for i in range(COLS) for j in range(i + 1)]
    outer = np.zeros((40, HISTORY_MOST), np.float32)
    for at, (i, j) in enumerate(lower):
        outer[at] = design[:HISTORY_MOST, i] * design[:HISTORY_MOST, j]
    by_chip = design.reshape(chips, chip_rows, COLS)
    vmem = pl.BlockSpec(memory_space=pltpu.VMEM)
    hbm = pl.BlockSpec(memory_space=pl.ANY)
    smem = pl.BlockSpec(memory_space=pltpu.SMEM)
    f32, i32, dma = jnp.float32, jnp.int32, pltpu.SemaphoreType.DMA
    scratch = [
        pltpu.VMEM((chip_rows, half), f32),
        pltpu.VMEM((chip_rows, pixels // 32), i32),
        pltpu.VMEM((chip_rows, half), f32),
        pltpu.VMEM((chip_rows, half), f32),
        pltpu.VMEM((chip_rows, pixels // 32), i32),
        pltpu.VMEM((HISTORY_MOST, 128), i32),
        pltpu.VMEM((hist, COLS, own), f32),
        pltpu.VMEM((hist, COLS, own), f32),
        pltpu.VMEM((40, own), f32),
        pltpu.VMEM((hist, COLS, own), f32),
        pltpu.VMEM((1, own), f32),
        pltpu.VMEM((hist, 1, own), f32),
        pltpu.VMEM((hist, 1, own), f32),
        pltpu.VMEM((1, half), f32),
        pltpu.VMEM((max(back - 1, 1), 1, half), f32),
        pltpu.VMEM((1, own), f32),
        pltpu.VMEM((2, late, 1, own), f32),
        pltpu.VMEM((chip_rows, half), f32),
        pltpu.VMEM((hist, 1, own), f32),
        pltpu.VMEM((late, hist, 1, own), f32),
        pltpu.VMEM((rows, half), f32),
        pltpu.VMEM((rows, half), f32),
        pltpu.VMEM((chip_rows, COLS), f32),
        pltpu.VMEM((chip_rows, COLS), f32),
        pltpu.VMEM((40, HISTORY_MOST), f32),
    ]
    for number in (2, 2 * hist, 2, 2 * hist, hist, hist, 1, hist, max(back - 1, 1), 2 * late, hist * late, hist, hist):
        scratch += [dma((number,)), dma((number,))]
    scratch.append(dma((6,)))
    return pl.pallas_call(
        functools.partial(fused_kernel, narrow, chips, hist, back),
        out_shape=[jax.ShapeDtypeStruct((rows, pixels), f32)] * 2,
        in_specs=[smem, smem, smem, vmem, vmem, hbm, hbm],
        out_specs=[vmem, vmem],
        scratch_shapes=scratch,
        compiler_params=pltpu.CompilerParams(has_side_effects=True),
    )(
        history_len, monitor_start, boundary_table, values, cloud_words,
        jnp.asarray(by_chip), jnp.asarray(outer),
    )


def fits(narrow, devices, rows, pixels):
    chip_rows = 2 * rows
    if narrow % 2 or rows % 8 or HISTORY_MOST % chip_rows or WINDOW % chip_rows:
        return False
    hist = HISTORY_MOST // chip_rows
    return devices // 2 == 2 * hist and (pixels // 2) % (hist * 128) == 0 and 128 % (pixels // 64 // hist) == 0


def solution(mesh):
    narrow = mesh.shape["narrow"]
    devices = narrow * mesh.shape["wide"]

    def per_device_any(values, *rest):
        if fits(narrow, devices, *values.shape):
            return fused_device(narrow, devices, values, *rest)
        return per_device(values, *rest)

    placed = (P(("wide", "narrow"), None), P(("wide", "narrow"), None), P(), P(), P())
    return jax.shard_map(
        per_device_any,
        mesh=mesh,
        in_specs=placed,
        out_specs=(P(("wide", "narrow"), None), P(("wide", "narrow"), None)),
        check_vma=False,
    )
```
